128 devices in a mesh: stage: 2 (over core), expert: 64 (over z, y, x).
Axes of the slice: x: 4, y: 4, z: 4, core: 2. Of those that a mesh axis runs over, the one named last changes fastest.
Arguments:
- x_act: bfloat16 [2, 32768, 256], P('stage', 'expert')
- route_idx: int32 [2, 32768, 2], P('stage', 'expert')
- route_gate: float32 [2, 32768, 2], P('stage', 'expert')
- w_up: bfloat16 [2, 64, 256, 2048], P('stage', 'expert')
- w_lin: bfloat16 [2, 64, 256, 2048], P('stage', 'expert')
- w_down: bfloat16 [2, 64, 2048, 256], P('stage', 'expert')
- dy_out: bfloat16 [2, 32768, 256], P('stage', 'expert')
Outputs:
- output 1: bfloat16 [2, 32768, 256], P('stage', 'expert')
- output 2: bfloat16 [2, 32768, 256], P('stage', 'expert')
- output 3: bfloat16 [2, 64, 256, 2048], P('stage', 'expert')
- output 4: bfloat16 [2, 64, 256, 2048], P('stage', 'expert')
- output 5: bfloat16 [2, 64, 2048, 256], P('stage', 'expert')
All inputs are finite; a program needn't handle non-finite values.
Results may differ from the reference program's by a relative error of at most 0.001.
Values are sent between devices in bfloat16 or wider.
A program may use at most 1 GiB of HBM per device.

```python
import jax
import jax.numpy as jnp
from jax import lax

STAGE_DEVS = 2
EXPERT_DEVS = 64
TOKENS = 512
D_MODEL = 256
D_FF = 2048
EXPERTS = 64
TOP_K = 2

CAPACITY = 4 * TOKENS // EXPERTS
ROWS = EXPERT_DEVS * TOKENS


def draw_routing(rng_key):
    key_hot, key_bias, key_cell, key_perm, key_swap = jax.random.split(rng_key, 5)
    num_cells = EXPERTS * CAPACITY
    cell_ids = jnp.arange(num_cells, dtype=jnp.int32)
    cell_expert = cell_ids // CAPACITY
    cell_slot = cell_ids % CAPACITY
    hot_expert = jax.random.randint(key_hot, (), 0, EXPERTS)
    expert_bias = jax.random.randint(key_bias, (EXPERTS,), 0, 4) * 256
    cell_score = jax.random.randint(key_cell, (num_cells,), 0, 1024) + expert_bias[cell_expert]
    needed = (cell_slot == 0) | (cell_expert == hot_expert)
    cell_score = jnp.where(needed, 4096, cell_score)
    top_vals, chosen = lax.top_k(cell_score * num_cells + cell_ids, 2 * TOKENS)
    chosen_expert = jnp.sort(chosen) // CAPACITY
    expert_pairs = jnp.stack([chosen_expert[:TOKENS], chosen_expert[TOKENS:]], axis=1)
    expert_pairs = expert_pairs[jax.random.permutation(key_perm, TOKENS)]
    swap_flag = jax.random.randint(key_swap, (TOKENS, 1), 0, 2)
    return jnp.where(swap_flag == 1, expert_pairs[:, ::-1], expert_pairs).astype(jnp.int32)


def setup_inputs(seed: int = 0) -> dict:
    root_key = jax.random.key(seed)
    key_x, key_route, key_gate, key_up, key_lin, key_down, key_dy = jax.random.split(root_key, 7)
    shape_tok = (STAGE_DEVS, ROWS, D_MODEL)
    x_act = jax.random.normal(key_x, shape_tok, jnp.float32).astype(jnp.bfloat16)
    route_keys = jax.random.split(key_route, STAGE_DEVS * EXPERT_DEVS)
    route_idx = jax.vmap(draw_routing)(route_keys).reshape(STAGE_DEVS, ROWS, TOP_K)
    first_gate = jax.random.uniform(key_gate, (STAGE_DEVS, ROWS, 1), jnp.float32, 0.3, 0.7)
    route_gate = jnp.concatenate([first_gate, 1.0 - first_gate], axis=-1)
    shape_in = (STAGE_DEVS, EXPERTS, D_MODEL, D_FF)
    shape_out = (STAGE_DEVS, EXPERTS, D_FF, D_MODEL)
    w_up = (jax.random.normal(key_up, shape_in, jnp.float32) * D_MODEL ** -0.5).astype(jnp.bfloat16)
    w_lin = (jax.random.normal(key_lin, shape_in, jnp.float32) * D_MODEL ** -0.5).astype(jnp.bfloat16)
    w_down = (jax.random.normal(key_down, shape_out, jnp.float32) * D_FF ** -0.5).astype(jnp.bfloat16)
    dy_out = jax.random.normal(key_dy, shape_tok, jnp.float32).astype(jnp.bfloat16)
    return {"x_act": x_act, "route_idx": route_idx, "route_gate": route_gate, "w_up": w_up, "w_lin": w_lin, "w_down": w_down, "dy_out": dy_out}


def expert_block(x_src, idx_src, gate_src, dy_dst, w_up, w_lin, w_down):
    member = jnp.sum(jax.nn.one_hot(idx_src, EXPERTS, dtype=jnp.int32), axis=1)
    earlier = jnp.cumsum(member, axis=0) - member
    slot_pos = jnp.take_along_axis(earlier, idx_src, axis=1)
    x_copies = jnp.broadcast_to(x_src.astype(jnp.float32)[:, None, :], (TOKENS, TOP_K, D_MODEL))
    empty_rows = jnp.zeros((EXPERTS, CAPACITY, D_MODEL), jnp.float32)
    x_rows = empty_rows.at[idx_src, slot_pos].set(x_copies)
    pre_up = jnp.einsum("ecd,edf->ecf", x_rows, w_up)
    pre_lin = jnp.einsum("ecd,edf->ecf", x_rows, w_lin)
    act_up = jax.nn.silu(pre_up)
    hidden = (act_up * pre_lin).astype(jnp.bfloat16).astype(jnp.float32)
    out_rows = jnp.einsum("ecf,efd->ecd", hidden, w_down).astype(jnp.bfloat16).astype(jnp.float32)
    out_copies = out_rows[idx_src, slot_pos]
    y_tok = jnp.sum(gate_src[:, :, None] * out_copies, axis=1).astype(jnp.bfloat16)
    d_copies = (gate_src[:, :, None] * dy_dst.astype(jnp.float32)[:, None, :]).astype(jnp.bfloat16).astype(jnp.float32)
    d_rows = empty_rows.at[idx_src, slot_pos].set(d_copies)
    d_hidden = jnp.einsum("ecd,efd->ecf", d_rows, w_down).astype(jnp.bfloat16).astype(jnp.float32)
    sigmoid_up = jax.nn.sigmoid(pre_up)
    d_up = (d_hidden * pre_lin * sigmoid_up * (1.0 + pre_up * (1.0 - sigmoid_up))).astype(jnp.bfloat16).astype(jnp.float32)
    d_lin = (d_hidden * act_up).astype(jnp.bfloat16).astype(jnp.float32)
    g_up = jnp.einsum("ecd,ecf->edf", x_rows, d_up)
    g_lin = jnp.einsum("ecd,ecf->edf", x_rows, d_lin)
    g_down = jnp.einsum("ecf,ecd->efd", hidden, d_rows)
    dx_rows = (jnp.einsum("ecf,edf->ecd", d_up, w_up) + jnp.einsum("ecf,edf->ecd", d_lin, w_lin)).astype(jnp.bfloat16).astype(jnp.float32)
    dx_tok = jnp.sum(dx_rows[idx_src, slot_pos], axis=1).astype(jnp.bfloat16)
    return y_tok, dx_tok, g_up, g_lin, g_down


def stage_block(stage_args):
    x_stage, idx_stage, gate_stage, dy_stage, w_up, w_lin, w_down = stage_args
    w_up32 = w_up.astype(jnp.float32)
    w_lin32 = w_lin.astype(jnp.float32)
    w_down32 = w_down.astype(jnp.float32)

    def device_step(grad_sums, dev_block):
        block_out = expert_block(dev_block[0], dev_block[1], dev_block[2], dev_block[3], w_up32, w_lin32, w_down32)
        new_sums = (grad_sums[0] + block_out[2], grad_sums[1] + block_out[3], grad_sums[2] + block_out[4])
        return new_sums, (block_out[0], block_out[1])

    zero_grads = (jnp.zeros((EXPERTS, D_MODEL, D_FF), jnp.float32), jnp.zeros((EXPERTS, D_MODEL, D_FF), jnp.float32), jnp.zeros((EXPERTS, D_FF, D_MODEL), jnp.float32))
    dev_blocks = (x_stage.reshape(EXPERT_DEVS, TOKENS, D_MODEL), idx_stage.reshape(EXPERT_DEVS, TOKENS, TOP_K), gate_stage.reshape(EXPERT_DEVS, TOKENS, TOP_K), dy_stage.reshape(EXPERT_DEVS, TOKENS, D_MODEL))
    grad_sums, tok_outs = lax.scan(device_step, zero_grads, dev_blocks)
    y_stage = tok_outs[0].reshape(ROWS, D_MODEL)
    dx_stage = tok_outs[1].reshape(ROWS, D_MODEL)
    return y_stage, dx_stage, grad_sums[0].astype(jnp.bfloat16), grad_sums[1].astype(jnp.bfloat16), grad_sums[2].astype(jnp.bfloat16)


def reference(x_act, route_idx, route_gate, w_up, w_lin, w_down, dy_out):
    x_from = jnp.roll(x_act, 1, axis=0)
    idx_from = jnp.roll(route_idx, 1, axis=0)
    gate_from = jnp.roll(route_gate, 1, axis=0)
    y_out, dx_next, dw_up, dw_lin, dw_down = lax.map(stage_block, (x_from, idx_from, gate_from, dy_out, w_up, w_lin, w_down))
    dx_act = jnp.roll(dx_next, -1, axis=0)
    return y_out, dx_act, dw_up, dw_lin, dw_down
```

```python
import functools

import jax
import jax.numpy as jnp
from jax import lax
from jax.experimental import pallas as pl
from jax.experimental.pallas import tpu as pltpu
from jax.sharding import PartitionSpec as P

MESH = pl.DeviceIdType.MESH
F32 = jnp.float32
BF16 = jnp.bfloat16
CAP = 32
GRP = 8
ROWS = GRP * CAP
FT = 256
NT = (((1,), (1,)), ((), ()))
TN = (((0,), (0,)), ((), ()))


def torus_step(pos, q, sign):
    a, b, c = lax.div(q, 16), lax.rem(lax.div(q, 4), 4), lax.rem(q, 4)
    step_x, step_y, step_z = c, lax.rem(c + a, 4), lax.rem(c + b, 4)
    if sign < 0:
        step_x, step_y, step_z = 4 - step_x, 4 - step_y, 4 - step_z
    z = lax.rem(lax.div(pos, 16) + step_z, 4)
    y = lax.rem(lax.rem(lax.div(pos, 4), 4) + step_y, 4)
    x = lax.rem(lax.rem(pos, 4) + step_x, 4)
    return z * 16 + y * 4 + x


def slot_ids(me, group, shape, dim):
    n = lax.broadcasted_iota(jnp.int32, shape, dim)
    q = n // CAP + group * GRP
    a, b, c = q >> 4, (q >> 2) & 3, q & 3
    z = (me // 16 + c + b) & 3
    y = (me // 4 + c + a) & 3
    x = (me + c) & 3
    return ((z * 16 + y * 4 + x) * CAP + (n & (CAP - 1))).astype(F32)


def moe_kernel(
    idx_hbm, gate_hbm, x_hbm, dy_hbm, wup_hbm, wlin_hbm, wdn_hbm,
    y_hbm, dx_hbm, gup_hbm, glin_hbm, gdn_hbm,
    idx_v, gate_v, x_v, dy_v, wup, wlin, wdn,
    xs, xr, us, ur, os, orr, ds, dr,
    hid, dup, dlin, own, par, col_own, col_par,
    sum0, sum1, sumx, gup, glin, gdn, y_v, dx_v,
    in_sem, out_sem, send_sem, x_sem, u_sem, o_sem, d_sem, pack_sem,
):
    me = lax.axis_index("expert")
    stage = lax.axis_index("stage")
    other = 1 - stage
    tokens = x_v.shape[0]
    experts = wup_experts = 64
    groups = experts // GRP
    ff = wup.shape[1]

    loads = [
        pltpu.make_async_copy(src, dst, in_sem.at[n])
        for n, (src, dst) in enumerate(
            ((idx_hbm, idx_v), (x_hbm, x_v), (gate_hbm, gate_v), (dy_hbm, dy_v), (wup_hbm, wup), (wlin_hbm, wlin), (wdn_hbm, wdn))
        )
    ]
    for load in loads:
        load.start()

    barrier = pltpu.get_barrier_semaphore()

    def greet(q, carry):
        peer = torus_step(me, q, 1)
        pl.semaphore_signal(barrier, inc=1, device_id=(other, peer), device_id_type=MESH)

        @pl.when(q > 0)
        def _():
            pl.semaphore_signal(barrier, inc=1, device_id=(stage, peer), device_id_type=MESH)

        return carry

    lax.fori_loop(0, experts, greet, 0)

    def copy_of(src, dst, kind, sem, group, place, dest_stage, sign):
        q = group * GRP + place
        rows = pl.ds(pl.multiple_of(q * CAP, CAP), CAP)
        return pltpu.make_async_remote_copy(
            src_ref=src.at[rows],
            dst_ref=dst.at[rows],
            send_sem=send_sem.at[kind],
            recv_sem=sem.at[group],
            device_id=(dest_stage, torus_step(me, q, sign)),
            device_id_type=MESH,
        )

    def send_group(src, dst, kind, sem, group, dest_stage, sign, skip_self):
        for place in range(GRP):
            if place == 0 and skip_self:

                @pl.when(group > 0)
                def _():
                    copy_of(src, dst, kind, sem, group, 0, dest_stage, sign).start()
            else:
                copy_of(src, dst, kind, sem, group, place, dest_stage, sign).start()

    def wait_rows(buf, sem, rows):
        pltpu.make_async_copy(buf.at[pl.ds(0, rows)], buf.at[pl.ds(0, rows)], sem).wait()

    def wait_group(buf, sem, group, skip_self):
        if not skip_self:
            wait_rows(buf, sem.at[group], ROWS)
            return

        @pl.when(group == 0)
        def _():
            wait_rows(buf, sem.at[0], ROWS - CAP)

        @pl.when(group > 0)
        def _():
            wait_rows(buf, sem.at[group], ROWS)

    send_x = functools.partial(send_group, xs, xr, 0, x_sem, dest_stage=other, sign=1, skip_self=False)
    send_u = functools.partial(send_group, us, ur, 1, u_sem, dest_stage=stage, sign=1, skip_self=True)
    send_o = functools.partial(send_group, os, orr, 2, o_sem, dest_stage=stage, sign=-1, skip_self=True)
    send_d = functools.partial(send_group, ds, dr, 3, d_sem, dest_stage=other, sign=-1, skip_self=False)

    loads[0].wait()
    expert_row = lax.broadcasted_iota(jnp.int32, (experts, tokens), 0)
    chosen = [(idx_v[pl.ds(j, 1), :] == expert_row).astype(F32) for j in range(2)]
    before = lax.broadcasted_iota(jnp.int32, (tokens, tokens), 0) < lax.broadcasted_iota(jnp.int32, (tokens, tokens), 1)
    earlier = jnp.dot(
        (chosen[0] + chosen[1]).astype(BF16), jnp.where(before, 1.0, 0.0).astype(BF16), preferred_element_type=F32
    )
    place = earlier + CAP * expert_row.astype(F32)
    loads[2].wait()
    for j in range(2):
        own[pl.ds(j, 1), :] = jnp.sum(chosen[j] * place, axis=0, keepdims=True)
        own[pl.ds(2 + j, 1), :] = gate_v[pl.ds(j, 1), :]
    own[pl.ds(4, 4), :] = jnp.zeros((4, tokens), F32)

    def slot_mask(route, group):
        slots = slot_ids(me, group, (ROWS, 128), 0)
        slots = jnp.concatenate([slots] * (tokens // 128), axis=1)
        return [slots == route[pl.ds(j, 1), :] for j in range(2)]

    def rows_of(group):
        return pl.ds(pl.multiple_of(group * ROWS, ROWS), ROWS)

    def x_block(group):
        hit = slot_mask(own, group)
        pick = jnp.where(hit[0] | hit[1], 1.0, 0.0).astype(BF16)
        xs[rows_of(group), :] = jnp.dot(pick, x_v[...], preferred_element_type=F32).astype(BF16)

    def u_block(group):
        hit = slot_mask(par, group)
        pick = jnp.where(hit[0] | hit[1], 1.0, 0.0).astype(BF16)
        gates = jnp.where(hit[0], par[pl.ds(2, 1), :], 0.0) + jnp.where(hit[1], par[pl.ds(3, 1), :], 0.0)
        gates = jnp.sum(gates, axis=1, keepdims=True)
        rows = jnp.dot(pick, dy_v[...], preferred_element_type=F32)
        us[rows_of(group), :] = (gates * rows).astype(BF16)

    loads[1].wait()
    x_block(0)
    x_block(1)
    pl.semaphore_wait(barrier, 2 * experts - 1)
    pack = pltpu.make_async_remote_copy(
        src_ref=own, dst_ref=par, send_sem=pack_sem.at[0], recv_sem=pack_sem.at[1],
        device_id=(other, me), device_id_type=MESH,
    )
    pack.start()
    send_x(0)
    x_block(2)
    send_x(1)
    loads[3].wait()
    pack.wait()

    def feed(group, carry):
        u_block(group)

        @pl.when(group + 3 < groups)
        def _():
            x_block(group + 3)

        @pl.when(group + 2 < groups)
        def _():
            send_x(group + 2)

        @pl.when(group > 0)
        def _():
            send_u(group - 1)

        @pl.when(group == 0)
        def _():
            ur[pl.ds(0, CAP), :] = us[pl.ds(0, CAP), :]

        return carry

    lax.fori_loop(0, groups, feed, 0)

    for route, cols, count in ((own, col_own, 2), (par, col_par, 4)):
        wide = jnp.concatenate([route[...], jnp.zeros((120, tokens), F32)], axis=0)
        tall = jnp.transpose(wide, (1, 0))
        for j in range(count):
            cols[j] = jnp.broadcast_to(tall[:, j : j + 1], (tokens, 128))
    send_u(groups - 1)
    for n in range(4, 7):
        loads[n].wait()

    def work(group, carry):
        rows = rows_of(group)
        wait_group(xr, x_sem, group, False)
        wait_group(ur, u_sem, group, True)
        x_in, u_in = xr[rows, :], ur[rows, :]
        for n in range(ff // FT):
            cols = pl.ds(n * FT, FT)
            pre_up = jnp.dot(x_in, wup[:, cols], preferred_element_type=F32)
            pre_lin = jnp.dot(x_in, wlin[:, cols], preferred_element_type=F32)
            d_hid = lax.dot_general(u_in, wdn[cols, :], NT, preferred_element_type=F32).astype(BF16).astype(F32)
            sig = jax.nn.sigmoid(pre_up)
            act = pre_up * sig
            hid[rows, cols] = (act * pre_lin).astype(BF16)
            dup[rows, cols] = (d_hid * pre_lin * sig * (1.0 + pre_up * (1.0 - sig))).astype(BF16)
            dlin[rows, cols] = (d_hid * act).astype(BF16)
        os[rows, :] = jnp.dot(hid[rows, :], wdn[...], preferred_element_type=F32).astype(BF16)

        @pl.when(group == 0)
        def _():
            orr[pl.ds(0, CAP), :] = os[pl.ds(0, CAP), :]

        d_in = lax.dot_general(dup[rows, :], wup[...], NT, preferred_element_type=F32)
        d_in += lax.dot_general(dlin[rows, :], wlin[...], NT, preferred_element_type=F32)
        send_o(group)
        ds[rows, :] = d_in.astype(BF16)

        @pl.when(group > 0)
        def _():
            send_d(group - 1)

        return carry

    lax.fori_loop(0, groups, work, 0)

    def weight_grads(n, carry):
        cols = pl.ds(pl.multiple_of(n * 256, 256), 256)
        gup[:, cols] = lax.dot_general(xr[...], dup[:, cols], TN, preferred_element_type=F32).astype(BF16)
        glin[:, cols] = lax.dot_general(xr[...], dlin[:, cols], TN, preferred_element_type=F32).astype(BF16)
        g_t = lax.dot_general(ur[...], hid[:, cols], TN, preferred_element_type=F32)
        gdn[cols, :] = jnp.transpose(g_t, (1, 0)).astype(BF16)

        @pl.when(n == 0)
        def _():
            send_d(groups - 1)

        return carry

    lax.fori_loop(0, ff // 256, weight_grads, 0)
    stores = [
        pltpu.make_async_copy(src, dst, out_sem.at[n])
        for n, (src, dst) in enumerate(((gup, gup_hbm), (glin, glin_hbm), (gdn, gdn_hbm), (y_v, y_hbm), (dx_v, dx_hbm)))
    ]
    for n in range(3):
        stores[n].start()

    sum0[...] = jnp.zeros_like(sum0)
    sum1[...] = jnp.zeros_like(sum1)
    sumx[...] = jnp.zeros_like(sumx)

    def merge(group, carry):
        rows = rows_of(group)
        slots = slot_ids(me, group, (8, ROWS), 1)[0:1, :]

        def token_mask(cols, j):
            return jnp.concatenate([cols[j]] * (ROWS // 128), axis=1) == slots

        wait_group(orr, o_sem, group, True)
        for j, total in enumerate((sum0, sum1)):
            pick = jnp.where(token_mask(col_par, j), 1.0, 0.0).astype(BF16)
            total[...] += jnp.dot(pick, orr[rows, :], preferred_element_type=F32)
        wait_group(dr, d_sem, group, False)
        pick = jnp.where(token_mask(col_own, 0) | token_mask(col_own, 1), 1.0, 0.0).astype(BF16)
        sumx[...] += jnp.dot(pick, dr[rows, :], preferred_element_type=F32)
        return carry

    lax.fori_loop(0, groups, merge, 0)
    g0 = jnp.concatenate([col_par[2]] * 2, axis=1)
    g1 = jnp.concatenate([col_par[3]] * 2, axis=1)
    y_v[...] = (g0 * sum0[...] + g1 * sum1[...]).astype(BF16)
    dx_v[...] = sumx[...].astype(BF16)
    stores[3].start()
    stores[4].start()
    wait_rows(xs, send_sem.at[0], experts * CAP)
    wait_rows(us, send_sem.at[1], (experts - 1) * CAP)
    wait_rows(os, send_sem.at[2], (experts - 1) * CAP)
    wait_rows(ds, send_sem.at[3], experts * CAP)
    for store in stores:
        store.wait()


def solution(mesh):
    tok_spec = P("stage", "expert", None)
    w_spec = P("stage", "expert", None, None)

    def device_step(x_act, route_idx, route_gate, w_up, w_lin, w_down, dy_out):
        _, tokens, width = x_act.shape
        ff = w_up.shape[3]
        slots = 64 * CAP
        groups = 64 // GRP
        any_spec = pl.BlockSpec(memory_space=pl.ANY)
        rows_buf = pltpu.VMEM((slots, width), BF16)
        ff_buf = pltpu.VMEM((slots, ff), BF16)
        dma = pltpu.SemaphoreType.DMA
        outs = pl.pallas_call(
            moe_kernel,
            name="moe",
            out_shape=(
                jax.ShapeDtypeStruct((tokens, width), BF16),
                jax.ShapeDtypeStruct((tokens, width), BF16),
                jax.ShapeDtypeStruct((width, ff), BF16),
                jax.ShapeDtypeStruct((width, ff), BF16),
                jax.ShapeDtypeStruct((ff, width), BF16),
            ),
            in_specs=[any_spec] * 7,
            out_specs=(any_spec,) * 5,
            scratch_shapes=[
                pltpu.VMEM((2, tokens), jnp.int32),
                pltpu.VMEM((2, tokens), F32),
                pltpu.VMEM((tokens, width), BF16),
                pltpu.VMEM((tokens, width), BF16),
                pltpu.VMEM((width, ff), BF16),
                pltpu.VMEM((width, ff), BF16),
                pltpu.VMEM((ff, width), BF16),
                *([rows_buf] * 8),
                *([ff_buf] * 3),
                pltpu.VMEM((8, tokens), F32),
                pltpu.VMEM((8, tokens), F32),
                pltpu.VMEM((2, tokens, 128), F32),
                pltpu.VMEM((4, tokens, 128), F32),
                *([pltpu.VMEM((tokens, width), F32)] * 3),
                pltpu.VMEM((width, ff), BF16),
                pltpu.VMEM((width, ff), BF16),
                pltpu.VMEM((ff, width), BF16),
                pltpu.VMEM((tokens, width), BF16),
                pltpu.VMEM((tokens, width), BF16),
                dma((7,)),
                dma((5,)),
                dma((4,)),
                dma((groups,)),
                dma((groups,)),
                dma((groups,)),
                dma((groups,)),
                dma((2,)),
            ],
            compiler_params=pltpu.CompilerParams(
                collective_id=0, has_side_effects=True, vmem_limit_bytes=66_000_000
            ),
        )(
            jnp.transpose(route_idx[0]), jnp.transpose(route_gate[0]), x_act[0], dy_out[0],
            w_up[0, 0], w_lin[0, 0], w_down[0, 0],
        )
        y_tok, dx_tok, g_up, g_lin, g_down = outs
        return y_tok[None], dx_tok[None], g_up[None, None], g_lin[None, None], g_down[None, None]

    return jax.shard_map(
        device_step,
        mesh=mesh,
        in_specs=(tok_spec, tok_spec, tok_spec, w_spec, w_spec, w_spec, tok_spec),
        out_specs=(tok_spec, tok_spec, w_spec, w_spec, w_spec),
        check_vma=False,
    )
```

```python
import functools

import jax
import jax.numpy as jnp
from jax import lax
from jax.experimental import pallas as pl
from jax.experimental.pallas import tpu as pltpu
from jax.sharding import PartitionSpec as P

MESH = pl.DeviceIdType.MESH
F32 = jnp.float32
BF16 = jnp.bfloat16
CAP = 32
GRP = 8
ROWS = GRP * CAP
FT = 256
RB = 32
NT = (((1,), (1,)), ((), ()))
TN = (((0,), (0,)), ((), ()))


def group_peers(me, group, sign):
    z, y, x = lax.div(me, 16), lax.rem(lax.div(me, 4), 4), lax.rem(me, 4)
    a = lax.div(group, 2)
    b = 2 * (group - 2 * a)
    along_x = [lax.rem(x + 8 + sign * k, 4) for k in range(4)]
    along_y = [4 * lax.rem(y + 8 + sign * (a + k), 4) for k in range(4)]
    along_z = [16 * lax.rem(z + 8 + sign * (b + k), 4) for k in range(4)]
    return [along_x[n % 4] + along_y[n % 4] + along_z[(n % 4 + n // 4) % 4] for n in range(GRP)]


def slot_ids(me, group, shape, dim):
    n = lax.broadcasted_iota(jnp.int32, shape, dim)
    q = n // CAP + group * GRP
    a, b, c = q >> 4, (q >> 2) & 3, q & 3
    z = (me // 16 + c + b) & 3
    y = (me // 4 + c + a) & 3
    x = (me + c) & 3
    return ((z * 16 + y * 4 + x) * CAP + (n & (CAP - 1))).astype(F32)


def moe_kernel(
    idx_hbm, gate_hbm, x_hbm, dy_hbm, wup_hbm, wlin_hbm, wdn_hbm,
    sum0, sum1, sumx, par, gup, glin, gdn,
    idx_v, gate_v, x_v, dy_v, wup, wlin, wdn,
    xs, xr, us, ur, os, orr, ds, dr,
    hid, dup, dlin, x_t, u_t, own, pick_x, pick_0, pick_1,
    in_sem, send_sem, x_sem, u_sem, o_sem, d_sem, pack_sem,
):
    me = lax.axis_index("expert")
    stage = lax.axis_index("stage")
    other = 1 - stage
    tokens = x_v.shape[0]
    experts = 64
    groups = experts // GRP
    ff = wup.shape[1]

    loads = [
        pltpu.make_async_copy(src, dst, in_sem.at[n])
        for n, (src, dst) in enumerate(
            ((idx_hbm, idx_v), (x_hbm, x_v), (gate_hbm, gate_v), (dy_hbm, dy_v), (wup_hbm, wup), (wlin_hbm, wlin), (wdn_hbm, wdn))
        )
    ]
    for load in loads:
        load.start()

    barrier = pltpu.get_barrier_semaphore()

    pl.semaphore_signal(barrier, inc=1, device_id=(other, me), device_id_type=MESH)

    def greet(n, carry):
        for k in range(7):
            peer = me + (n * 7 + k + 1)
            peer = peer - jnp.where(peer >= experts, experts, 0)
            for side in (stage, other):
                pl.semaphore_signal(barrier, inc=1, device_id=(side, peer), device_id_type=MESH)
        return carry

    lax.fori_loop(0, experts // 7, greet, 0)

    def send_group(src, dst, kind, sem, group, dest_stage, sign, skip_self):
        peers = group_peers(me, jnp.int32(group), sign)
        for place in range(GRP):
            if place == 0 and skip_self and isinstance(group, int) and group == 0:
                continue
            rows = pl.ds(pl.multiple_of((group * GRP + place) * CAP, CAP), CAP)
            pltpu.make_async_remote_copy(
                src_ref=src.at[rows],
                dst_ref=dst.at[rows],
                send_sem=send_sem.at[kind],
                recv_sem=sem.at[group],
                device_id=(dest_stage, peers[place]),
                device_id_type=MESH,
            ).start()

    def wait_rows(buf, sem, rows):
        pltpu.make_async_copy(buf.at[pl.ds(0, rows)], buf.at[pl.ds(0, rows)], sem).wait()

    def wait_group(buf, sem, group, skip_self):
        own_slot = skip_self and isinstance(group, int) and group == 0
        wait_rows(buf, sem.at[group], ROWS - CAP if own_slot else ROWS)

    send_x = functools.partial(send_group, xs, xr, 0, x_sem, dest_stage=other, sign=1, skip_self=False)
    send_u = functools.partial(send_group, us, ur, 1, u_sem, dest_stage=stage, sign=1, skip_self=True)
    send_o = functools.partial(send_group, os, orr, 2, o_sem, dest_stage=stage, sign=-1, skip_self=True)
    send_d = functools.partial(send_group, ds, dr, 3, d_sem, dest_stage=other, sign=-1, skip_self=False)

    loads[0].wait()
    expert_row = lax.broadcasted_iota(jnp.int32, (experts, tokens), 0)
    chosen = [(idx_v[pl.ds(j, 1), :] == expert_row).astype(F32) for j in range(2)]
    before = lax.broadcasted_iota(jnp.int32, (tokens, tokens), 0) < lax.broadcasted_iota(jnp.int32, (tokens, tokens), 1)
    earlier = jnp.dot(
        (chosen[0] + chosen[1]).astype(BF16), jnp.where(before, 1.0, 0.0).astype(BF16), preferred_element_type=F32
    )
    place = earlier + CAP * expert_row.astype(F32)
    loads[2].wait()
    for j in range(2):
        own[pl.ds(j, 1), :] = jnp.sum(chosen[j] * place, axis=0, keepdims=True)
        own[pl.ds(2 + j, 1), :] = gate_v[pl.ds(j, 1), :]
    own[pl.ds(4, 4), :] = jnp.zeros((4, tokens), F32)

    def slot_mask(route, group):
        slots = slot_ids(me, group, (ROWS, 128), 0)
        slots = jnp.concatenate([slots] * (tokens // 128), axis=1)
        return [slots == route[pl.ds(j, 1), :] for j in range(2)]

    def rows_of(group):
        return pl.ds(pl.multiple_of(group * ROWS, ROWS), ROWS)

    def x_block(group):
        rows = rows_of(group)
        hit = slot_mask(own, group)
        pick = jnp.where(hit[0] | hit[1], 1.0, 0.0).astype(BF16)
        pick_x[rows, :] = pick
        xs[rows, :] = jnp.dot(pick, x_v[...], preferred_element_type=F32).astype(BF16)

    def u_block(group):
        rows = rows_of(group)
        hit = slot_mask(par, group)
        picks = [jnp.where(h, 1.0, 0.0) for h in hit]
        gates = picks[0] * par[pl.ds(2, 1), :] + picks[1] * par[pl.ds(3, 1), :]
        gates = jnp.sum(gates, axis=1, keepdims=True)
        pick_0[rows, :] = picks[0].astype(BF16)
        pick_1[rows, :] = picks[1].astype(BF16)
        pick = (picks[0] + picks[1]).astype(BF16)
        us[rows, :] = (gates * jnp.dot(pick, dy_v[...], preferred_element_type=F32)).astype(BF16)

    loads[1].wait()
    x_block(0)
    x_block(1)
    pl.semaphore_wait(barrier, 2 * experts - 1)
    pack = pltpu.make_async_remote_copy(
        src_ref=own, dst_ref=par, send_sem=pack_sem.at[0], recv_sem=pack_sem.at[1],
        device_id=(other, me), device_id_type=MESH,
    )
    pack.start()
    send_x(0)
    x_block(2)
    send_x(1)
    loads[3].wait()
    pack.wait()
    u_block(0)
    ur[pl.ds(0, CAP), :] = us[pl.ds(0, CAP), :]
    x_block(3)
    send_x(2)
    send_u(0)

    def feed(group, carry):
        u_block(group)
        x_block(group + 3)
        send_x(group + 2)

        @pl.when(group > 1)
        def _():
            send_u(group - 1)

        return carry

    lax.fori_loop(1, groups - 3, feed, 0)

    def feed_u(group, carry):
        send_u(group - 1)
        u_block(group)
        return carry

    send_x(groups - 1)
    lax.fori_loop(groups - 3, groups, feed_u, 0)
    for n in range(4, 7):
        loads[n].wait()
    send_u(groups - 1)

    def work(group):
        rows = rows_of(group)
        wait_group(xr, x_sem, group, False)
        wait_group(ur, u_sem, group, True)
        x_in, u_in = xr[rows, :], ur[rows, :]
        x_t[:, rows] = jnp.transpose(x_in, (1, 0))
        u_t[:, rows] = jnp.transpose(u_in, (1, 0))
        for n in range(ff // FT):
            cols = pl.ds(n * FT, FT)
            all_up = jnp.dot(x_in, wup[:, cols], preferred_element_type=F32)
            all_lin = jnp.dot(x_in, wlin[:, cols], preferred_element_type=F32)
            all_d = lax.dot_general(u_in, wdn[cols, :], NT, preferred_element_type=F32)
            for r in range(0, ROWS, RB):
                part = pl.ds(pl.multiple_of(group * ROWS + r, RB), RB)
                pre_up, pre_lin = all_up[r : r + RB], all_lin[r : r + RB]
                d_hid = all_d[r : r + RB].astype(BF16).astype(F32)
                sig = jax.nn.sigmoid(pre_up)
                act = pre_up * sig
                hid[part, cols] = (act * pre_lin).astype(BF16)
                dup[part, cols] = (d_hid * pre_lin * sig * (1.0 + pre_up * (1.0 - sig))).astype(BF16)
                dlin[part, cols] = (d_hid * act).astype(BF16)
        os[rows, :] = jnp.dot(hid[rows, :], wdn[...], preferred_element_type=F32).astype(BF16)
        d_in = lax.dot_general(dup[rows, :], wup[...], NT, preferred_element_type=F32)
        d_in += lax.dot_general(dlin[rows, :], wlin[...], NT, preferred_element_type=F32)
        send_o(group)
        ds[rows, :] = d_in.astype(BF16)

    work(0)
    orr[pl.ds(0, CAP), :] = os[pl.ds(0, CAP), :]

    def work_next(group, carry):
        work(group)
        send_d(group - 1)
        return carry

    lax.fori_loop(1, groups, work_next, 0)

    def weight_grads(n, carry):
        cols = pl.ds(pl.multiple_of(n * 256, 256), 256)
        gup[:, cols] = jnp.dot(x_t[...], dup[:, cols], preferred_element_type=F32).astype(BF16)
        glin[:, cols] = jnp.dot(x_t[...], dlin[:, cols], preferred_element_type=F32).astype(BF16)
        gdn[cols, :] = jnp.transpose(jnp.dot(u_t[...], hid[:, cols], preferred_element_type=F32), (1, 0)).astype(BF16)
        return carry

    weight_grads(0, 0)
    send_d(groups - 1)
    lax.fori_loop(1, ff // 256, weight_grads, 0)

    def merge(group, first):
        rows = rows_of(group)

        def add(total, rows_in, pick):
            part = lax.dot_general(rows_in, pick, TN, preferred_element_type=F32)
            total[...] = part if first else total[...] + part

        wait_group(orr, o_sem, group, True)
        rows_o = orr[rows, :]
        add(sum0, rows_o, pick_0[rows, :])
        add(sum1, rows_o, pick_1[rows, :])
        wait_group(dr, d_sem, group, False)
        add(sumx, dr[rows, :], pick_x[rows, :])

    merge(0, True)

    def merge_next(group, carry):
        merge(group, False)
        return carry

    lax.fori_loop(1, groups, merge_next, 0)
    wait_rows(xs, send_sem.at[0], experts * CAP)
    wait_rows(us, send_sem.at[1], (experts - 1) * CAP)
    wait_rows(os, send_sem.at[2], (experts - 1) * CAP)
    wait_rows(ds, send_sem.at[3], experts * CAP)


def finish_kernel(
    sum0, sum1, sumx, route, gup, glin, gdn,
    y_hbm, dx_hbm, gup_hbm, glin_hbm, gdn_hbm, y_v, dx_v, sem,
):
    pairs = ((gup, gup_hbm), (glin, glin_hbm), (gdn, gdn_hbm), (y_v, y_hbm), (dx_v, dx_hbm))
    stores = [pltpu.make_async_copy(src, dst, sem.at[n]) for n, (src, dst) in enumerate(pairs)]
    for n in range(3):
        stores[n].start()
    y_t = route[pl.ds(2, 1), :] * sum0[...] + route[pl.ds(3, 1), :] * sum1[...]
    y_v[...] = jnp.transpose(y_t, (1, 0)).astype(BF16)
    stores[3].start()
    dx_v[...] = jnp.transpose(sumx[...], (1, 0)).astype(BF16)
    stores[4].start()
    for store in stores:
        store.wait()


def solution(mesh):
    tok_spec = P("stage", "expert", None)
    w_spec = P("stage", "expert", None, None)

    def device_step(x_act, route_idx, route_gate, w_up, w_lin, w_down, dy_out):
        _, tokens, width = x_act.shape
        ff = w_up.shape[3]
        slots = 64 * CAP
        groups = 64 // GRP
        any_spec = pl.BlockSpec(memory_space=pl.ANY)
        rows_buf = pltpu.VMEM((slots, width), BF16)
        ff_buf = pltpu.VMEM((slots, ff), BF16)
        dma = pltpu.SemaphoreType.DMA
        any_specs = [any_spec] * 5
        vmem_spec = pl.BlockSpec(memory_space=pltpu.VMEM)
        held = pl.pallas_call(
            moe_kernel,
            name="moe",
            out_shape=(
                *([pltpu.VMEM((width, tokens), F32)] * 3),
                pltpu.VMEM((8, tokens), F32),
                pltpu.VMEM((width, ff), BF16),
                pltpu.VMEM((width, ff), BF16),
                pltpu.VMEM((ff, width), BF16),
            ),
            in_specs=[any_spec] * 7,
            out_specs=(vmem_spec,) * 7,
            scratch_shapes=[
                pltpu.VMEM((2, tokens), jnp.int32),
                pltpu.VMEM((2, tokens), F32),
                pltpu.VMEM((tokens, width), BF16),
                pltpu.VMEM((tokens, width), BF16),
                pltpu.VMEM((width, ff), BF16),
                pltpu.VMEM((width, ff), BF16),
                pltpu.VMEM((ff, width), BF16),
                *([rows_buf] * 8),
                *([ff_buf] * 3),
                *([pltpu.VMEM((width, slots), BF16)] * 2),
                pltpu.VMEM((8, tokens), F32),
                *([pltpu.VMEM((slots, tokens), BF16)] * 3),
                dma((7,)),
                dma((4,)),
                dma((groups,)),
                dma((groups,)),
                dma((groups,)),
                dma((groups,)),
                dma((2,)),
            ],
            compiler_params=pltpu.CompilerParams(
                collective_id=0, has_side_effects=True, vmem_limit_bytes=56 * 2**20
            ),
        )(
            jnp.transpose(route_idx[0]), jnp.transpose(route_gate[0]), x_act[0], dy_out[0],
            w_up[0, 0], w_lin[0, 0], w_down[0, 0],
        )
        outs = pl.pallas_call(
            finish_kernel,
            name="finish",
            out_shape=(
                jax.ShapeDtypeStruct((tokens, width), BF16),
                jax.ShapeDtypeStruct((tokens, width), BF16),
                jax.ShapeDtypeStruct((width, ff), BF16),
                jax.ShapeDtypeStruct((width, ff), BF16),
                jax.ShapeDtypeStruct((ff, width), BF16),
            ),
            in_specs=[vmem_spec] * 7,
            out_specs=any_specs,
            scratch_shapes=[pltpu.VMEM((tokens, width), BF16), pltpu.VMEM((tokens, width), BF16), dma((5,))],
            compiler_params=pltpu.CompilerParams(vmem_limit_bytes=4 * 2**20),
        )(*held)
        y_tok, dx_tok, g_up, g_lin, g_down = outs
        return y_tok[None], dx_tok[None], g_up[None, None], g_lin[None, None], g_down[None, None]

    return jax.shard_map(
        device_step,
        mesh=mesh,
        in_specs=(tok_spec, tok_spec, tok_spec, w_spec, w_spec, w_spec, tok_spec),
        out_specs=(tok_spec, tok_spec, w_spec, w_spec, w_spec),
        check_vma=False,
    )
```

```python
import functools

import jax
import jax.numpy as jnp
from jax import lax
from jax.experimental import pallas as pl
from jax.experimental.pallas import tpu as pltpu
from jax.sharding import PartitionSpec as P

MESH = pl.DeviceIdType.MESH
F32 = jnp.float32
BF16 = jnp.bfloat16
CAP = 32
GRP = 8
ROWS = GRP * CAP
FT = 256
RB = 32
HOLD = 5
AHEAD = 4
NT = (((1,), (1,)), ((), ()))
TN = (((0,), (0,)), ((), ()))


def group_peers(me, group, sign):
    z, y, x = lax.div(me, 16), lax.rem(lax.div(me, 4), 4), lax.rem(me, 4)
    a = lax.div(group, 2)
    b = 2 * (group - 2 * a)
    along_x = [lax.rem(x + 8 + sign * k, 4) for k in range(4)]
    along_y = [4 * lax.rem(y + 8 + sign * (a + k), 4) for k in range(4)]
    along_z = [16 * lax.rem(z + 8 + sign * (b + k), 4) for k in range(4)]
    return [along_x[n % 4] + along_y[n % 4] + along_z[(n % 4 + n // 4) % 4] for n in range(GRP)]


def slot_ids(me, group, shape, dim):
    n = lax.broadcasted_iota(jnp.int32, shape, dim)
    q = n // CAP + group * GRP
    a, b, c = q >> 4, (q >> 2) & 3, q & 3
    z = (me // 16 + c + b) & 3
    y = (me // 4 + c + a) & 3
    x = (me + c) & 3
    return ((z * 16 + y * 4 + x) * CAP + (n & (CAP - 1))).astype(F32)


def moe_kernel(
    idx_hbm, gate_hbm, x_hbm, dy_hbm, wup_hbm, wlin_hbm, wdn_hbm,
    sum0, sum1, sumx, par, gup, glin, gdn,
    idx_v, gate_v, x_v, dy_v, wup, wlin, wdn,
    xs, xr, us, ur, os, orr, ds, dr,
    hid, dup, dlin, x_t, u_t, own, pick_x, pick_0, pick_1,
    in_sem, send_sem, x_sem, u_sem, o_sem, d_sem, pack_sem,
):
    me = lax.axis_index("expert")
    stage = lax.axis_index("stage")
    other = 1 - stage
    tokens = x_v.shape[0]
    experts = 64
    groups = experts // GRP
    ff = wup.shape[1]

    loads = [
        pltpu.make_async_copy(src, dst, in_sem.at[n])
        for n, (src, dst) in enumerate(
            ((idx_hbm, idx_v), (x_hbm, x_v), (gate_hbm, gate_v), (dy_hbm, dy_v), (wup_hbm, wup), (wlin_hbm, wlin), (wdn_hbm, wdn))
        )
    ]
    for load in loads:
        load.start()

    barrier = pltpu.get_barrier_semaphore()

    z, y, x = lax.div(me, 16), lax.rem(lax.div(me, 4), 4), lax.rem(me, 4)
    ring = [[lax.rem(pos + k, 4) * unit for k in range(4)] for pos, unit in ((z, 16), (y, 4), (x, 1))]
    hops = (0, 1, 2, 1)
    steps = [(i, j, k) for i in range(4) for j in range(4) for k in range(4)]
    for i, j, k in sorted(steps, key=lambda n: -sum(hops[m] for m in n)):
        peer = ring[0][i] + ring[1][j] + ring[2][k]
        for side in (stage, other):
            if (i, j, k) != (0, 0, 0) or side is other:
                pl.semaphore_signal(barrier, inc=1, device_id=(side, peer), device_id_type=MESH)

    def send_group(src, dst, kind, sem, group, dest_stage, sign, skip_self):
        peers = group_peers(me, jnp.int32(group), sign)
        for place in range(GRP):
            if place == 0 and skip_self and isinstance(group, int) and group == 0:
                continue
            rows = pl.ds(pl.multiple_of((group * GRP + place) * CAP, CAP), CAP)
            pltpu.make_async_remote_copy(
                src_ref=src.at[rows],
                dst_ref=dst.at[rows],
                send_sem=send_sem.at[kind],
                recv_sem=sem.at[group],
                device_id=(dest_stage, peers[place]),
                device_id_type=MESH,
            ).start()

    def wait_rows(buf, sem, rows):
        pltpu.make_async_copy(buf.at[pl.ds(0, rows)], buf.at[pl.ds(0, rows)], sem).wait()

    def wait_group(buf, sem, group, skip_self):
        own_slot = skip_self and isinstance(group, int) and group == 0
        wait_rows(buf, sem.at[group], ROWS - CAP if own_slot else ROWS)

    send_x = functools.partial(send_group, xs, xr, 0, x_sem, dest_stage=other, sign=1, skip_self=False)
    send_u = functools.partial(send_group, us, ur, 1, u_sem, dest_stage=stage, sign=1, skip_self=True)
    send_o = functools.partial(send_group, os, orr, 2, o_sem, dest_stage=stage, sign=-1, skip_self=True)
    send_d = functools.partial(send_group, ds, dr, 3, d_sem, dest_stage=other, sign=-1, skip_self=False)

    loads[0].wait()
    expert_row = lax.broadcasted_iota(jnp.int32, (experts, tokens), 0)
    chosen = [(idx_v[pl.ds(j, 1), :] == expert_row).astype(F32) for j in range(2)]
    before = lax.broadcasted_iota(jnp.int32, (tokens, tokens), 0) < lax.broadcasted_iota(jnp.int32, (tokens, tokens), 1)
    earlier = jnp.dot(
        (chosen[0] + chosen[1]).astype(BF16), jnp.where(before, 1.0, 0.0).astype(BF16), preferred_element_type=F32
    )
    place = earlier + CAP * expert_row.astype(F32)
    loads[2].wait()
    for j in range(2):
        own[pl.ds(j, 1), :] = jnp.sum(chosen[j] * place, axis=0, keepdims=True)
        own[pl.ds(2 + j, 1), :] = gate_v[pl.ds(j, 1), :]
    own[pl.ds(4, 4), :] = jnp.zeros((4, tokens), F32)

    def slot_mask(route, group):
        slots = slot_ids(me, group, (ROWS, 128), 0)
        slots = jnp.concatenate([slots] * (tokens // 128), axis=1)
        return [slots == route[pl.ds(j, 1), :] for j in range(2)]

    def rows_of(group):
        return pl.ds(pl.multiple_of(group * ROWS, ROWS), ROWS)

    def x_block(group):
        rows = rows_of(group)
        hit = slot_mask(own, group)
        pick = jnp.where(hit[0] | hit[1], 1.0, 0.0).astype(BF16)
        pick_x[rows, :] = pick
        xs[rows, :] = jnp.dot(pick, x_v[...], preferred_element_type=F32).astype(BF16)

    def u_block(group):
        rows = rows_of(group)
        hit = slot_mask(par, group)
        picks = [jnp.where(h, 1.0, 0.0) for h in hit]
        gates = picks[0] * par[pl.ds(2, 1), :] + picks[1] * par[pl.ds(3, 1), :]
        gates = jnp.sum(gates, axis=1, keepdims=True)
        pick_0[rows, :] = picks[0].astype(BF16)
        pick_1[rows, :] = picks[1].astype(BF16)
        pick = (picks[0] + picks[1]).astype(BF16)
        us[rows, :] = (gates * jnp.dot(pick, dy_v[...], preferred_element_type=F32)).astype(BF16)

    loads[1].wait()
    x_block(0)
    x_block(1)
    pl.semaphore_wait(barrier, 2 * experts - 1)
    pack = pltpu.make_async_remote_copy(
        src_ref=own, dst_ref=par, send_sem=pack_sem.at[0], recv_sem=pack_sem.at[1],
        device_id=(other, me), device_id_type=MESH,
    )
    pack.start()
    send_x(0)
    x_block(2)
    send_x(1)
    loads[3].wait()
    pack.wait()
    for group in range(AHEAD):
        u_block(group)
        if group == 0:
            ur[pl.ds(0, CAP), :] = us[pl.ds(0, CAP), :]
        if group + 3 < groups:
            x_block(group + 3)
        if group + 2 < AHEAD:
            send_x(group + 2)
        send_u(group)

    def feed(group, carry):
        u_block(group)

        @pl.when(group + 3 < groups)
        def _():
            x_block(group + 3)

        return carry

    lax.fori_loop(AHEAD, groups, feed, 0)
    for n in range(4, 7):
        loads[n].wait()

    def work(group, send):
        rows = rows_of(group)
        wait_group(xr, x_sem, group, False)
        wait_group(ur, u_sem, group, True)
        if isinstance(group, int):
            if group + AHEAD < groups:
                send_x(group + AHEAD)
                send_u(group + AHEAD)
        elif AHEAD < groups:

            @pl.when(group + AHEAD < groups)
            def _():
                send_x(group + AHEAD)
                send_u(group + AHEAD)

        x_in, u_in = xr[rows, :], ur[rows, :]
        x_t[:, rows] = jnp.transpose(x_in, (1, 0))
        u_t[:, rows] = jnp.transpose(u_in, (1, 0))
        for n in range(ff // FT):
            cols = pl.ds(n * FT, FT)
            all_up = jnp.dot(x_in, wup[:, cols], preferred_element_type=F32)
            all_lin = jnp.dot(x_in, wlin[:, cols], preferred_element_type=F32)
            all_d = lax.dot_general(u_in, wdn[cols, :], NT, preferred_element_type=F32)
            for r in range(0, ROWS, RB):
                part = pl.ds(pl.multiple_of(group * ROWS + r, RB), RB)
                pre_up, pre_lin = all_up[r : r + RB], all_lin[r : r + RB]
                d_hid = all_d[r : r + RB].astype(BF16).astype(F32)
                sig = jax.nn.sigmoid(pre_up)
                act = pre_up * sig
                hid[part, cols] = (act * pre_lin).astype(BF16)
                dup[part, cols] = (d_hid * pre_lin * sig * (1.0 + pre_up * (1.0 - sig))).astype(BF16)
                dlin[part, cols] = (d_hid * act).astype(BF16)
        os[rows, :] = jnp.dot(hid[rows, :], wdn[...], preferred_element_type=F32).astype(BF16)
        d_in = lax.dot_general(dup[rows, :], wup[...], NT, preferred_element_type=F32)
        d_in += lax.dot_general(dlin[rows, :], wlin[...], NT, preferred_element_type=F32)
        if send:
            send_o(group)
        ds[rows, :] = d_in.astype(BF16)

    work(0, False)
    orr[pl.ds(0, CAP), :] = os[pl.ds(0, CAP), :]

    def work_hold(group, carry):
        work(group, False)
        return carry

    def release(group, carry):
        send_o(group)
        send_d(group)
        return carry

    def work_next(group, carry):
        work(group, True)
        send_d(group - 1)
        return carry

    lax.fori_loop(1, HOLD, work_hold, 0)
    release(0, 0)
    lax.fori_loop(1, HOLD - 1, release, 0)
    send_o(HOLD - 1)
    lax.fori_loop(HOLD, groups, work_next, 0)

    def weight_grads(n, carry):
        cols = pl.ds(pl.multiple_of(n * 256, 256), 256)
        gup[:, cols] = jnp.dot(x_t[...], dup[:, cols], preferred_element_type=F32).astype(BF16)
        glin[:, cols] = jnp.dot(x_t[...], dlin[:, cols], preferred_element_type=F32).astype(BF16)
        gdn[cols, :] = jnp.transpose(jnp.dot(u_t[...], hid[:, cols], preferred_element_type=F32), (1, 0)).astype(BF16)
        return carry

    weight_grads(0, 0)
    send_d(groups - 1)
    lax.fori_loop(1, ff // 256, weight_grads, 0)

    def merge(lo, hi):
        rows = pl.ds(lo * ROWS, (hi - lo) * ROWS)

        def add(total, buf, pick):
            part = lax.dot_general(buf[rows, :], pick[rows, :], TN, preferred_element_type=F32)
            total[...] = part if lo == 0 else total[...] + part

        for group in range(lo, hi):
            wait_group(orr, o_sem, group, True)
        add(sum0, orr, pick_0)
        add(sum1, orr, pick_1)
        for group in range(lo, hi):
            wait_group(dr, d_sem, group, False)
        add(sumx, dr, pick_x)

    merge(0, 4)
    merge(4, groups)
    wait_rows(xs, send_sem.at[0], experts * CAP)
    wait_rows(us, send_sem.at[1], (experts - 1) * CAP)
    wait_rows(os, send_sem.at[2], (experts - 1) * CAP)
    wait_rows(ds, send_sem.at[3], experts * CAP)


def finish_kernel(
    sum0, sum1, sumx, route, gup, glin, gdn,
    y_hbm, dx_hbm, gup_hbm, glin_hbm, gdn_hbm, y_v, dx_v, sem,
):
    pairs = ((gup, gup_hbm), (glin, glin_hbm), (gdn, gdn_hbm), (y_v, y_hbm), (dx_v, dx_hbm))
    stores = [pltpu.make_async_copy(src, dst, sem.at[n]) for n, (src, dst) in enumerate(pairs)]
    for n in range(3):
        stores[n].start()
    y_t = route[pl.ds(2, 1), :] * sum0[...] + route[pl.ds(3, 1), :] * sum1[...]
    y_v[...] = jnp.transpose(y_t, (1, 0)).astype(BF16)
    stores[3].start()
    dx_v[...] = jnp.transpose(sumx[...], (1, 0)).astype(BF16)
    stores[4].start()
    for store in stores:
        store.wait()


def solution(mesh):
    tok_spec = P("stage", "expert", None)
    w_spec = P("stage", "expert", None, None)

    def device_step(x_act, route_idx, route_gate, w_up, w_lin, w_down, dy_out):
        _, tokens, width = x_act.shape
        ff = w_up.shape[3]
        slots = 64 * CAP
        groups = 64 // GRP
        any_spec = pl.BlockSpec(memory_space=pl.ANY)
        rows_buf = pltpu.VMEM((slots, width), BF16)
        ff_buf = pltpu.VMEM((slots, ff), BF16)
        dma = pltpu.SemaphoreType.DMA
        any_specs = [any_spec] * 5
        vmem_spec = pl.BlockSpec(memory_space=pltpu.VMEM)
        held = pl.pallas_call(
            moe_kernel,
            name="moe",
            out_shape=(
                *([pltpu.VMEM((width, tokens), F32)] * 3),
                pltpu.VMEM((8, tokens), F32),
                pltpu.VMEM((width, ff), BF16),
                pltpu.VMEM((width, ff), BF16),
                pltpu.VMEM((ff, width), BF16),
            ),
            in_specs=[any_spec] * 7,
            out_specs=(vmem_spec,) * 7,
            scratch_shapes=[
                pltpu.VMEM((2, tokens), jnp.int32),
                pltpu.VMEM((2, tokens), F32),
                pltpu.VMEM((tokens, width), BF16),
                pltpu.VMEM((tokens, width), BF16),
                pltpu.VMEM((width, ff), BF16),
                pltpu.VMEM((width, ff), BF16),
                pltpu.VMEM((ff, width), BF16),
                *([rows_buf] * 8),
                *([ff_buf] * 3),
                *([pltpu.VMEM((width, slots), BF16)] * 2),
                pltpu.VMEM((8, tokens), F32),
                *([pltpu.VMEM((slots, tokens), BF16)] * 3),
                dma((7,)),
                dma((4,)),
                dma((groups,)),
                dma((groups,)),
                dma((groups,)),
                dma((groups,)),
                dma((2,)),
            ],
            compiler_params=pltpu.CompilerParams(
                collective_id=0, has_side_effects=True, vmem_limit_bytes=56 * 2**20
            ),
        )(
            jnp.transpose(route_idx[0]), jnp.transpose(route_gate[0]), x_act[0], dy_out[0],
            w_up[0, 0], w_lin[0, 0], w_down[0, 0],
        )
        outs = pl.pallas_call(
            finish_kernel,
            name="finish",
            out_shape=(
                jax.ShapeDtypeStruct((tokens, width), BF16),
                jax.ShapeDtypeStruct((tokens, width), BF16),
                jax.ShapeDtypeStruct((width, ff), BF16),
                jax.ShapeDtypeStruct((width, ff), BF16),
                jax.ShapeDtypeStruct((ff, width), BF16),
            ),
            in_specs=[vmem_spec] * 7,
            out_specs=any_specs,
            scratch_shapes=[pltpu.VMEM((tokens, width), BF16), pltpu.VMEM((tokens, width), BF16), dma((5,))],
            compiler_params=pltpu.CompilerParams(vmem_limit_bytes=4 * 2**20),
        )(*held)
        y_tok, dx_tok, g_up, g_lin, g_down = outs
        return y_tok[None], dx_tok[None], g_up[None, None], g_lin[None, None], g_down[None, None]

    return jax.shard_map(
        device_step,
        mesh=mesh,
        in_specs=(tok_spec, tok_spec, tok_spec, w_spec, w_spec, w_spec, tok_spec),
        out_specs=(tok_spec, tok_spec, w_spec, w_spec, w_spec),
        check_vma=False,
    )
```

```python
import functools

import jax
import jax.numpy as jnp
from jax import lax
from jax.experimental import pallas as pl
from jax.experimental.pallas import tpu as pltpu
from jax.sharding import PartitionSpec as P

MESH = pl.DeviceIdType.MESH
F32 = jnp.float32
BF16 = jnp.bfloat16
CAP = 32
GRP = 8
ROWS = GRP * CAP
FT = 256
RB = 32
HOLD = 5
AHEAD = 6
NT = (((1,), (1,)), ((), ()))
TN = (((0,), (0,)), ((), ()))


def group_peers(me, group, sign):
    z, y, x = lax.div(me, 16), lax.rem(lax.div(me, 4), 4), lax.rem(me, 4)
    a = lax.div(group, 2)
    b = 2 * (group - 2 * a)
    along_x = [lax.rem(x + 8 + sign * k, 4) for k in range(4)]
    along_y = [4 * lax.rem(y + 8 + sign * (a + k), 4) for k in range(4)]
    along_z = [16 * lax.rem(z + 8 + sign * (b + k), 4) for k in range(4)]
    return [along_x[n % 4] + along_y[n % 4] + along_z[(n % 4 + n // 4) % 4] for n in range(GRP)]


def slot_ids(me, group, shape, dim):
    n = lax.broadcasted_iota(jnp.int32, shape, dim)
    q = n // CAP + group * GRP
    a, b, c = q >> 4, (q >> 2) & 3, q & 3
    z = (me // 16 + c + b) & 3
    y = (me // 4 + c + a) & 3
    x = (me + c) & 3
    return ((z * 16 + y * 4 + x) * CAP + (n & (CAP - 1))).astype(F32)


def moe_kernel(
    idx_hbm, gate_hbm, x_hbm, dy_hbm, wup_hbm, wlin_hbm, wdn_hbm,
    sum0, sum1, sumx, par, gup, glin, gdn,
    idx_v, gate_v, x_v, dy_v, wup, wlin, wdn,
    xs, xr, us, ur, os, orr, ds, dr,
    hid, dup, dlin, x_t, u_t, own, pick_x, pick_0, pick_1,
    in_sem, send_sem, x_sem, u_sem, o_sem, d_sem, pack_sem,
):
    me = lax.axis_index("expert")
    stage = lax.axis_index("stage")
    other = 1 - stage
    tokens = x_v.shape[0]
    experts = 64
    groups = experts // GRP
    ff = wup.shape[1]

    loads = [
        pltpu.make_async_copy(src, dst, in_sem.at[n])
        for n, (src, dst) in enumerate(
            ((idx_hbm, idx_v), (x_hbm, x_v), (gate_hbm, gate_v), (dy_hbm, dy_v), (wup_hbm, wup), (wlin_hbm, wlin), (wdn_hbm, wdn))
        )
    ]
    for load in loads:
        load.start()

    barrier = pltpu.get_barrier_semaphore()

    z, y, x = lax.div(me, 16), lax.rem(lax.div(me, 4), 4), lax.rem(me, 4)
    ring = [[lax.rem(pos + k, 4) * unit for k in range(4)] for pos, unit in ((z, 16), (y, 4), (x, 1))]
    hops = (0, 1, 2, 1)
    steps = [(i, j, k) for i in range(4) for j in range(4) for k in range(4)]
    for i, j, k in sorted(steps, key=lambda n: -sum(hops[m] for m in n)):
        peer = ring[0][i] + ring[1][j] + ring[2][k]
        for side in (stage, other):
            if (i, j, k) != (0, 0, 0) or side is other:
                pl.semaphore_signal(barrier, inc=1, device_id=(side, peer), device_id_type=MESH)

    def send_group(src, dst, kind, sem, group, dest_stage, sign, skip_self):
        peers = group_peers(me, jnp.int32(group), sign)
        for place in range(GRP):
            if place == 0 and skip_self and isinstance(group, int) and group == 0:
                continue
            rows = pl.ds(pl.multiple_of((group * GRP + place) * CAP, CAP), CAP)
            pltpu.make_async_remote_copy(
                src_ref=src.at[rows],
                dst_ref=dst.at[rows],
                send_sem=send_sem.at[kind],
                recv_sem=sem.at[group],
                device_id=(dest_stage, peers[place]),
                device_id_type=MESH,
            ).start()

    def wait_rows(buf, sem, rows):
        pltpu.make_async_copy(buf.at[pl.ds(0, rows)], buf.at[pl.ds(0, rows)], sem).wait()

    def wait_group(buf, sem, group, skip_self):
        own_slot = skip_self and isinstance(group, int) and group == 0
        wait_rows(buf, sem.at[group], ROWS - CAP if own_slot else ROWS)

    send_x = functools.partial(send_group, xs, xr, 0, x_sem, dest_stage=other, sign=1, skip_self=False)
    send_u = functools.partial(send_group, us, ur, 1, u_sem, dest_stage=stage, sign=1, skip_self=True)
    send_o = functools.partial(send_group, os, orr, 2, o_sem, dest_stage=stage, sign=-1, skip_self=True)
    send_d = functools.partial(send_group, ds, dr, 3, d_sem, dest_stage=other, sign=-1, skip_self=False)

    loads[0].wait()
    expert_row = lax.broadcasted_iota(jnp.int32, (experts, tokens), 0)
    chosen = [(idx_v[pl.ds(j, 1), :] == expert_row).astype(F32) for j in range(2)]
    before = lax.broadcasted_iota(jnp.int32, (tokens, tokens), 0) < lax.broadcasted_iota(jnp.int32, (tokens, tokens), 1)
    earlier = jnp.dot(
        (chosen[0] + chosen[1]).astype(BF16), jnp.where(before, 1.0, 0.0).astype(BF16), preferred_element_type=F32
    )
    place = earlier + CAP * expert_row.astype(F32)
    loads[2].wait()
    for j in range(2):
        own[pl.ds(j, 1), :] = jnp.sum(chosen[j] * place, axis=0, keepdims=True)
        own[pl.ds(2 + j, 1), :] = gate_v[pl.ds(j, 1), :]
    own[pl.ds(4, 4), :] = jnp.zeros((4, tokens), F32)

    def slot_mask(route, group):
        slots = slot_ids(me, group, (ROWS, 128), 0)
        slots = jnp.concatenate([slots] * (tokens // 128), axis=1)
        return [slots == route[pl.ds(j, 1), :] for j in range(2)]

    def rows_of(group):
        return pl.ds(pl.multiple_of(group * ROWS, ROWS), ROWS)

    def x_block(group):
        rows = rows_of(group)
        hit = slot_mask(own, group)
        pick = jnp.where(hit[0] | hit[1], 1.0, 0.0).astype(BF16)
        pick_x[rows, :] = pick
        xs[rows, :] = jnp.dot(pick, x_v[...], preferred_element_type=F32).astype(BF16)

    def u_block(group):
        rows = rows_of(group)
        hit = slot_mask(par, group)
        picks = [jnp.where(h, 1.0, 0.0) for h in hit]
        gates = picks[0] * par[pl.ds(2, 1), :] + picks[1] * par[pl.ds(3, 1), :]
        gates = jnp.sum(gates, axis=1, keepdims=True)
        pick_0[rows, :] = picks[0].astype(BF16)
        pick_1[rows, :] = picks[1].astype(BF16)
        pick = (picks[0] + picks[1]).astype(BF16)
        us[rows, :] = (gates * jnp.dot(pick, dy_v[...], preferred_element_type=F32)).astype(BF16)

    loads[1].wait()

    def fill_x(group, carry):
        x_block(group)
        return carry

    lax.fori_loop(0, groups, fill_x, 0)
    pl.semaphore_wait(barrier, 2 * experts - 1)
    pack = pltpu.make_async_remote_copy(
        src_ref=own, dst_ref=par, send_sem=pack_sem.at[0], recv_sem=pack_sem.at[1],
        device_id=(other, me), device_id_type=MESH,
    )
    pack.start()
    send_x(0)
    send_x(1)
    loads[3].wait()
    pack.wait()
    for group in range(AHEAD):
        u_block(group)
        if group == 0:
            ur[pl.ds(0, CAP), :] = us[pl.ds(0, CAP), :]
        if group > 0:
            send_u(group - 1)
        if 1 < group:
            send_x(group)

    def fill_u(group, carry):
        u_block(group)
        return carry

    u_block(AHEAD)
    send_u(AHEAD - 1)
    lax.fori_loop(AHEAD + 1, groups, fill_u, 0)
    for n in range(4, 7):
        loads[n].wait()

    def work(group, send):
        rows = rows_of(group)
        wait_group(xr, x_sem, group, False)
        wait_group(ur, u_sem, group, True)
        if isinstance(group, int):
            if group + AHEAD < groups:
                send_x(group + AHEAD)
                send_u(group + AHEAD)
        elif AHEAD < groups:

            @pl.when(group + AHEAD < groups)
            def _():
                send_x(group + AHEAD)
                send_u(group + AHEAD)

        x_in, u_in = xr[rows, :], ur[rows, :]
        x_t[:, rows] = jnp.transpose(x_in, (1, 0))
        u_t[:, rows] = jnp.transpose(u_in, (1, 0))
        for n in range(ff // FT):
            cols = pl.ds(n * FT, FT)
            all_up = jnp.dot(x_in, wup[:, cols], preferred_element_type=F32)
            all_lin = jnp.dot(x_in, wlin[:, cols], preferred_element_type=F32)
            all_d = lax.dot_general(u_in, wdn[cols, :], NT, preferred_element_type=F32)
            for r in range(0, ROWS, RB):
                part = pl.ds(pl.multiple_of(group * ROWS + r, RB), RB)
                pre_up, pre_lin = all_up[r : r + RB], all_lin[r : r + RB]
                d_hid = all_d[r : r + RB].astype(BF16).astype(F32)
                sig = jax.nn.sigmoid(pre_up)
                act = pre_up * sig
                hid[part, cols] = (act * pre_lin).astype(BF16)
                dup[part, cols] = (d_hid * pre_lin * sig * (1.0 + pre_up * (1.0 - sig))).astype(BF16)
                dlin[part, cols] = (d_hid * act).astype(BF16)
        os[rows, :] = jnp.dot(hid[rows, :], wdn[...], preferred_element_type=F32).astype(BF16)
        d_in = lax.dot_general(dup[rows, :], wup[...], NT, preferred_element_type=F32)
        d_in += lax.dot_general(dlin[rows, :], wlin[...], NT, preferred_element_type=F32)
        if send:
            send_o(group)
        ds[rows, :] = d_in.astype(BF16)

    work(0, False)
    orr[pl.ds(0, CAP), :] = os[pl.ds(0, CAP), :]

    def work_hold(group, carry):
        work(group, False)
        return carry

    def release(group):
        send_o(group)
        send_d(group)

    def work_next(group, carry):
        work(group, False)
        release(2 * group - 8)
        release(2 * group - 7)
        return carry

    lax.fori_loop(1, 4, work_hold, 0)
    work(4, False)
    for group in range(2):
        release(group)
    lax.fori_loop(4+1, groups, work_next, 0)

    def weight_grads(n, carry):
        cols = pl.ds(pl.multiple_of(n * 256, 256), 256)
        gup[:, cols] = jnp.dot(x_t[...], dup[:, cols], preferred_element_type=F32).astype(BF16)
        glin[:, cols] = jnp.dot(x_t[...], dlin[:, cols], preferred_element_type=F32).astype(BF16)
        gdn[cols, :] = jnp.transpose(jnp.dot(u_t[...], hid[:, cols], preferred_element_type=F32), (1, 0)).astype(BF16)
        return carry

    lax.fori_loop(0, ff // 256, weight_grads, 0)

    def merge(lo, hi):
        rows = pl.ds(lo * ROWS, (hi - lo) * ROWS)

        def add(total, buf, pick):
            part = lax.dot_general(buf[rows, :], pick[rows, :], TN, preferred_element_type=F32)
            total[...] = part if lo == 0 else total[...] + part

        for group in range(lo, hi):
            wait_group(orr, o_sem, group, True)
        add(sum0, orr, pick_0)
        add(sum1, orr, pick_1)
        for group in range(lo, hi):
            wait_group(dr, d_sem, group, False)
        add(sumx, dr, pick_x)

    merge(0, 4)
    merge(4, groups)
    wait_rows(xs, send_sem.at[0], experts * CAP)
    wait_rows(us, send_sem.at[1], (experts - 1) * CAP)
    wait_rows(os, send_sem.at[2], (experts - 1) * CAP)
    wait_rows(ds, send_sem.at[3], experts * CAP)


def finish_kernel(
    sum0, sum1, sumx, route, gup, glin, gdn,
    y_hbm, dx_hbm, gup_hbm, glin_hbm, gdn_hbm, y_v, dx_v, sem,
):
    pairs = ((gup, gup_hbm), (glin, glin_hbm), (gdn, gdn_hbm), (y_v, y_hbm), (dx_v, dx_hbm))
    stores = [pltpu.make_async_copy(src, dst, sem.at[n]) for n, (src, dst) in enumerate(pairs)]
    for n in range(3):
        stores[n].start()
    y_t = route[pl.ds(2, 1), :] * sum0[...] + route[pl.ds(3, 1), :] * sum1[...]
    y_v[...] = jnp.transpose(y_t, (1, 0)).astype(BF16)
    stores[3].start()
    dx_v[...] = jnp.transpose(sumx[...], (1, 0)).astype(BF16)
    stores[4].start()
    for store in stores:
        store.wait()


def solution(mesh):
    tok_spec = P("stage", "expert", None)
    w_spec = P("stage", "expert", None, None)

    def device_step(x_act, route_idx, route_gate, w_up, w_lin, w_down, dy_out):
        _, tokens, width = x_act.shape
        ff = w_up.shape[3]
        slots = 64 * CAP
        groups = 64 // GRP
        any_spec = pl.BlockSpec(memory_space=pl.ANY)
        rows_buf = pltpu.VMEM((slots, width), BF16)
        ff_buf = pltpu.VMEM((slots, ff), BF16)
        dma = pltpu.SemaphoreType.DMA
        any_specs = [any_spec] * 5
        vmem_spec = pl.BlockSpec(memory_space=pltpu.VMEM)
        held = pl.pallas_call(
            moe_kernel,
            name="moe",
            out_shape=(
                *([pltpu.VMEM((width, tokens), F32)] * 3),
                pltpu.VMEM((8, tokens), F32),
                pltpu.VMEM((width, ff), BF16),
                pltpu.VMEM((width, ff), BF16),
                pltpu.VMEM((ff, width), BF16),
            ),
            in_specs=[any_spec] * 7,
            out_specs=(vmem_spec,) * 7,
            scratch_shapes=[
                pltpu.VMEM((2, tokens), jnp.int32),
                pltpu.VMEM((2, tokens), F32),
                pltpu.VMEM((tokens, width), BF16),
                pltpu.VMEM((tokens, width), BF16),
                pltpu.VMEM((width, ff), BF16),
                pltpu.VMEM((width, ff), BF16),
                pltpu.VMEM((ff, width), BF16),
                *([rows_buf] * 8),
                *([ff_buf] * 3),
                *([pltpu.VMEM((width, slots), BF16)] * 2),
                pltpu.VMEM((8, tokens), F32),
                *([pltpu.VMEM((slots, tokens), BF16)] * 3),
                dma((7,)),
                dma((4,)),
                dma((groups,)),
                dma((groups,)),
                dma((groups,)),
                dma((groups,)),
                dma((2,)),
            ],
            compiler_params=pltpu.CompilerParams(
                collective_id=0, has_side_effects=True, vmem_limit_bytes=56 * 2**20
            ),
        )(
            jnp.transpose(route_idx[0]), jnp.transpose(route_gate[0]), x_act[0], dy_out[0],
            w_up[0, 0], w_lin[0, 0], w_down[0, 0],
        )
        outs = pl.pallas_call(
            finish_kernel,
            name="finish",
            out_shape=(
                jax.ShapeDtypeStruct((tokens, width), BF16),
                jax.ShapeDtypeStruct((tokens, width), BF16),
                jax.ShapeDtypeStruct((width, ff), BF16),
                jax.ShapeDtypeStruct((width, ff), BF16),
                jax.ShapeDtypeStruct((ff, width), BF16),
            ),
            in_specs=[vmem_spec] * 7,
            out_specs=any_specs,
            scratch_shapes=[pltpu.VMEM((tokens, width), BF16), pltpu.VMEM((tokens, width), BF16), dma((5,))],
            compiler_params=pltpu.CompilerParams(vmem_limit_bytes=4 * 2**20),
        )(*held)
        y_tok, dx_tok, g_up, g_lin, g_down = outs
        return y_tok[None], dx_tok[None], g_up[None, None], g_lin[None, None], g_down[None, None]

    return jax.shard_map(
        device_step,
        mesh=mesh,
        in_specs=(tok_spec, tok_spec, tok_spec, w_spec, w_spec, w_spec, tok_spec),
        out_specs=(tok_spec, tok_spec, w_spec, w_spec, w_spec),
        check_vma=False,
    )
```

```python
import functools

import jax
import jax.numpy as jnp
from jax import lax
from jax.experimental import pallas as pl
from jax.experimental.pallas import tpu as pltpu
from jax.sharding import PartitionSpec as P

MESH = pl.DeviceIdType.MESH
F32 = jnp.float32
BF16 = jnp.bfloat16
CAP = 32
GRP = 8
ROWS = GRP * CAP
FT = 256
RB = 32
HOLD = 5
AHEAD = 6
NT = (((1,), (1,)), ((), ()))
TN = (((0,), (0,)), ((), ()))


def group_peers(me, group, sign):
    z, y, x = lax.div(me, 16), lax.rem(lax.div(me, 4), 4), lax.rem(me, 4)
    a = lax.div(group, 2)
    b = 2 * (group - 2 * a)
    along_x = [lax.rem(x + 8 + sign * k, 4) for k in range(4)]
    along_y = [4 * lax.rem(y + 8 + sign * (a + k), 4) for k in range(4)]
    along_z = [16 * lax.rem(z + 8 + sign * (b + k), 4) for k in range(4)]
    return [along_x[n % 4] + along_y[n % 4] + along_z[(n % 4 + n // 4) % 4] for n in range(GRP)]


def slot_ids(me, group, shape, dim):
    n = lax.broadcasted_iota(jnp.int32, shape, dim)
    q = n // CAP + group * GRP
    a, b, c = q >> 4, (q >> 2) & 3, q & 3
    z = (me // 16 + c + b) & 3
    y = (me // 4 + c + a) & 3
    x = (me + c) & 3
    return ((z * 16 + y * 4 + x) * CAP + (n & (CAP - 1))).astype(F32)


def moe_kernel(
    idx_hbm, gate_hbm, x_hbm, dy_hbm, wup_hbm, wlin_hbm, wdn_hbm,
    sum0, sum1, sumx, par, gup, glin, gdn,
    idx_v, gate_v, x_v, dy_v, wup, wlin, wdn,
    xs, xr, us, ur, os, orr, ds, dr,
    hid, dup, dlin, x_t, u_t, own, pick_x, pick_0, pick_1,
    in_sem, send_sem, x_sem, u_sem, o_sem, d_sem, pack_sem,
):
    me = lax.axis_index("expert")
    stage = lax.axis_index("stage")
    other = 1 - stage
    tokens = x_v.shape[0]
    experts = 64
    groups = experts // GRP
    ff = wup.shape[1]

    loads = [
        pltpu.make_async_copy(src, dst, in_sem.at[n])
        for n, (src, dst) in enumerate(
            ((idx_hbm, idx_v), (x_hbm, x_v), (gate_hbm, gate_v), (dy_hbm, dy_v), (wup_hbm, wup), (wlin_hbm, wlin), (wdn_hbm, wdn))
        )
    ]
    for load in loads:
        load.start()

    barrier = pltpu.get_barrier_semaphore()

    z, y, x = lax.div(me, 16), lax.rem(lax.div(me, 4), 4), lax.rem(me, 4)
    ring = [[lax.rem(pos + k, 4) * unit for k in range(4)] for pos, unit in ((z, 16), (y, 4), (x, 1))]
    hops = (0, 1, 2, 1)
    steps = [(i, j, k) for i in range(4) for j in range(4) for k in range(4)]
    for i, j, k in sorted(steps, key=lambda n: -sum(hops[m] for m in n)):
        peer = ring[0][i] + ring[1][j] + ring[2][k]
        for side in (stage, other):
            if (i, j, k) != (0, 0, 0) or side is other:
                pl.semaphore_signal(barrier, inc=1, device_id=(side, peer), device_id_type=MESH)

    def send_group(src, dst, kind, sem, group, dest_stage, sign, skip_self):
        peers = group_peers(me, jnp.int32(group), sign)
        for place in range(GRP):
            if place == 0 and skip_self and isinstance(group, int) and group == 0:
                continue
            rows = pl.ds(pl.multiple_of((group * GRP + place) * CAP, CAP), CAP)
            pltpu.make_async_remote_copy(
                src_ref=src.at[rows],
                dst_ref=dst.at[rows],
                send_sem=send_sem.at[kind],
                recv_sem=sem.at[group],
                device_id=(dest_stage, peers[place]),
                device_id_type=MESH,
            ).start()

    def wait_rows(buf, sem, rows):
        pltpu.make_async_copy(buf.at[pl.ds(0, rows)], buf.at[pl.ds(0, rows)], sem).wait()

    def wait_group(buf, sem, group, skip_self):
        own_slot = skip_self and isinstance(group, int) and group == 0
        wait_rows(buf, sem.at[group], ROWS - CAP if own_slot else ROWS)

    send_x = functools.partial(send_group, xs, xr, 0, x_sem, dest_stage=other, sign=1, skip_self=False)
    send_u = functools.partial(send_group, us, ur, 1, u_sem, dest_stage=stage, sign=1, skip_self=True)
    send_o = functools.partial(send_group, os, orr, 2, o_sem, dest_stage=stage, sign=-1, skip_self=True)
    send_d = functools.partial(send_group, ds, dr, 3, d_sem, dest_stage=other, sign=-1, skip_self=False)

    loads[0].wait()
    expert_row = lax.broadcasted_iota(jnp.int32, (experts, tokens), 0)
    chosen = [(idx_v[pl.ds(j, 1), :] == expert_row).astype(F32) for j in range(2)]
    before = lax.broadcasted_iota(jnp.int32, (tokens, tokens), 0) < lax.broadcasted_iota(jnp.int32, (tokens, tokens), 1)
    earlier = jnp.dot(
        (chosen[0] + chosen[1]).astype(BF16), jnp.where(before, 1.0, 0.0).astype(BF16), preferred_element_type=F32
    )
    place = earlier + CAP * expert_row.astype(F32)
    loads[2].wait()
    for j in range(2):
        own[pl.ds(j, 1), :] = jnp.sum(chosen[j] * place, axis=0, keepdims=True)
        own[pl.ds(2 + j, 1), :] = gate_v[pl.ds(j, 1), :]
    own[pl.ds(4, 4), :] = jnp.zeros((4, tokens), F32)

    def slot_mask(route, group):
        slots = slot_ids(me, group, (ROWS, 128), 0)
        slots = jnp.concatenate([slots] * (tokens // 128), axis=1)
        return [slots == route[pl.ds(j, 1), :] for j in range(2)]

    def rows_of(group):
        return pl.ds(pl.multiple_of(group * ROWS, ROWS), ROWS)

    def x_block(group):
        rows = rows_of(group)
        hit = slot_mask(own, group)
        pick = jnp.where(hit[0] | hit[1], 1.0, 0.0).astype(BF16)
        pick_x[rows, :] = pick
        xs[rows, :] = jnp.dot(pick, x_v[...], preferred_element_type=F32).astype(BF16)

    def u_block(group):
        rows = rows_of(group)
        hit = slot_mask(par, group)
        picks = [jnp.where(h, 1.0, 0.0) for h in hit]
        gates = picks[0] * par[pl.ds(2, 1), :] + picks[1] * par[pl.ds(3, 1), :]
        gates = jnp.sum(gates, axis=1, keepdims=True)
        pick_0[rows, :] = picks[0].astype(BF16)
        pick_1[rows, :] = picks[1].astype(BF16)
        pick = (picks[0] + picks[1]).astype(BF16)
        us[rows, :] = (gates * jnp.dot(pick, dy_v[...], preferred_element_type=F32)).astype(BF16)

    loads[1].wait()

    def fill_x(group, carry):
        x_block(group)
        return carry

    lax.fori_loop(0, groups, fill_x, 0)
    pl.semaphore_wait(barrier, 2 * experts - 1)
    pack = pltpu.make_async_remote_copy(
        src_ref=own, dst_ref=par, send_sem=pack_sem.at[0], recv_sem=pack_sem.at[1],
        device_id=(other, me), device_id_type=MESH,
    )
    pack.start()
    send_x(0)
    send_x(1)
    loads[3].wait()
    pack.wait()
    for group in range(AHEAD):
        u_block(group)
        if group == 0:
            ur[pl.ds(0, CAP), :] = us[pl.ds(0, CAP), :]
        if group > 0:
            send_u(group - 1)
        if 1 < group:
            send_x(group)

    def fill_u(group, carry):
        u_block(group)
        return carry

    u_block(AHEAD)
    send_u(AHEAD - 1)
    lax.fori_loop(AHEAD + 1, groups, fill_u, 0)
    for n in range(4, 7):
        loads[n].wait()

    def work(group, send):
        rows = rows_of(group)
        wait_group(xr, x_sem, group, False)
        wait_group(ur, u_sem, group, True)
        if isinstance(group, int):
            if group + AHEAD < groups:
                send_x(group + AHEAD)
                send_u(group + AHEAD)
        elif AHEAD < groups:

            @pl.when(group + AHEAD < groups)
            def _():
                send_x(group + AHEAD)
                send_u(group + AHEAD)

        x_in, u_in = xr[rows, :], ur[rows, :]
        x_t[:, rows] = jnp.transpose(x_in, (1, 0))
        u_t[:, rows] = jnp.transpose(u_in, (1, 0))
        for n in range(ff // FT):
            cols = pl.ds(n * FT, FT)
            all_up = jnp.dot(x_in, wup[:, cols], preferred_element_type=F32)
            all_lin = jnp.dot(x_in, wlin[:, cols], preferred_element_type=F32)
            all_d = lax.dot_general(u_in, wdn[cols, :], NT, preferred_element_type=F32)
            for r in range(0, ROWS, RB):
                part = pl.ds(pl.multiple_of(group * ROWS + r, RB), RB)
                pre_up, pre_lin = all_up[r : r + RB], all_lin[r : r + RB]
                d_hid = all_d[r : r + RB].astype(BF16).astype(F32)
                sig = jax.nn.sigmoid(pre_up)
                act = pre_up * sig
                hid[part, cols] = (act * pre_lin).astype(BF16)
                dup[part, cols] = (d_hid * pre_lin * sig * (1.0 + pre_up * (1.0 - sig))).astype(BF16)
                dlin[part, cols] = (d_hid * act).astype(BF16)
        os[rows, :] = jnp.dot(hid[rows, :], wdn[...], preferred_element_type=F32).astype(BF16)
        d_in = lax.dot_general(dup[rows, :], wup[...], NT, preferred_element_type=F32)
        d_in += lax.dot_general(dlin[rows, :], wlin[...], NT, preferred_element_type=F32)
        if send:
            send_o(group)
        ds[rows, :] = d_in.astype(BF16)

    work(0, False)
    orr[pl.ds(0, CAP), :] = os[pl.ds(0, CAP), :]

    def work_hold(group, carry):
        work(group, False)
        return carry

    def release(group):
        send_o(group)
        send_d(group)

    def work_next(group, carry):
        work(group, False)
        release(2 * group - 8)
        release(2 * group - 7)
        return carry

    lax.fori_loop(1, 4, work_hold, 0)
    work(4, False)
    for group in range(2):
        release(group)
    lax.fori_loop(4+1, groups, work_next, 0)

    def weight_grads(n, carry):
        cols = pl.ds(pl.multiple_of(n * 256, 256), 256)
        gup[:, cols] = jnp.dot(x_t[...], dup[:, cols], preferred_element_type=F32).astype(BF16)
        glin[:, cols] = jnp.dot(x_t[...], dlin[:, cols], preferred_element_type=F32).astype(BF16)
        gdn[cols, :] = jnp.transpose(jnp.dot(u_t[...], hid[:, cols], preferred_element_type=F32), (1, 0)).astype(BF16)
        return carry

    lax.fori_loop(0, ff // 256, weight_grads, 0)

    def merge(lo, hi):
        rows = pl.ds(lo * ROWS, (hi - lo) * ROWS)

        def add(total, buf, pick):
            part = lax.dot_general(buf[rows, :], pick[rows, :], TN, preferred_element_type=F32)
            total[...] = part if lo == 0 else total[...] + part

        for group in range(lo, hi):
            wait_group(orr, o_sem, group, True)
        add(sum0, orr, pick_0)
        add(sum1, orr, pick_1)
        for group in range(lo, hi):
            wait_group(dr, d_sem, group, False)
        add(sumx, dr, pick_x)

    merge(0, 6)
    merge(6, groups)
    wait_rows(xs, send_sem.at[0], experts * CAP)
    wait_rows(us, send_sem.at[1], (experts - 1) * CAP)
    wait_rows(os, send_sem.at[2], (experts - 1) * CAP)
    wait_rows(ds, send_sem.at[3], experts * CAP)


def finish_kernel(
    sum0, sum1, sumx, route, gup, glin, gdn,
    y_hbm, dx_hbm, gup_hbm, glin_hbm, gdn_hbm, y_v, dx_v, sem,
):
    pairs = ((gup, gup_hbm), (glin, glin_hbm), (gdn, gdn_hbm), (y_v, y_hbm), (dx_v, dx_hbm))
    stores = [pltpu.make_async_copy(src, dst, sem.at[n]) for n, (src, dst) in enumerate(pairs)]
    for n in range(3):
        stores[n].start()
    y_t = route[pl.ds(2, 1), :] * sum0[...] + route[pl.ds(3, 1), :] * sum1[...]
    y_v[...] = jnp.transpose(y_t, (1, 0)).astype(BF16)
    stores[3].start()
    dx_v[...] = jnp.transpose(sumx[...], (1, 0)).astype(BF16)
    stores[4].start()
    for store in stores:
        store.wait()


def solution(mesh):
    tok_spec = P("stage", "expert", None)
    w_spec = P("stage", "expert", None, None)

    def device_step(x_act, route_idx, route_gate, w_up, w_lin, w_down, dy_out):
        _, tokens, width = x_act.shape
        ff = w_up.shape[3]
        slots = 64 * CAP
        groups = 64 // GRP
        any_spec = pl.BlockSpec(memory_space=pl.ANY)
        rows_buf = pltpu.VMEM((slots, width), BF16)
        ff_buf = pltpu.VMEM((slots, ff), BF16)
        dma = pltpu.SemaphoreType.DMA
        any_specs = [any_spec] * 5
        vmem_spec = pl.BlockSpec(memory_space=pltpu.VMEM)
        held = pl.pallas_call(
            moe_kernel,
            name="moe",
            out_shape=(
                *([pltpu.VMEM((width, tokens), F32)] * 3),
                pltpu.VMEM((8, tokens), F32),
                pltpu.VMEM((width, ff), BF16),
                pltpu.VMEM((width, ff), BF16),
                pltpu.VMEM((ff, width), BF16),
            ),
            in_specs=[any_spec] * 7,
            out_specs=(vmem_spec,) * 7,
            scratch_shapes=[
                pltpu.VMEM((2, tokens), jnp.int32),
                pltpu.VMEM((2, tokens), F32),
                pltpu.VMEM((tokens, width), BF16),
                pltpu.VMEM((tokens, width), BF16),
                pltpu.VMEM((width, ff), BF16),
                pltpu.VMEM((width, ff), BF16),
                pltpu.VMEM((ff, width), BF16),
                *([rows_buf] * 8),
                *([ff_buf] * 3),
                *([pltpu.VMEM((width, slots), BF16)] * 2),
                pltpu.VMEM((8, tokens), F32),
                *([pltpu.VMEM((slots, tokens), BF16)] * 3),
                dma((7,)),
                dma((4,)),
                dma((groups,)),
                dma((groups,)),
                dma((groups,)),
                dma((groups,)),
                dma((2,)),
            ],
            compiler_params=pltpu.CompilerParams(
                collective_id=0, has_side_effects=True, vmem_limit_bytes=56 * 2**20
            ),
        )(
            jnp.transpose(route_idx[0]), jnp.transpose(route_gate[0]), x_act[0], dy_out[0],
            w_up[0, 0], w_lin[0, 0], w_down[0, 0],
        )
        outs = pl.pallas_call(
            finish_kernel,
            name="finish",
            out_shape=(
                jax.ShapeDtypeStruct((tokens, width), BF16),
                jax.ShapeDtypeStruct((tokens, width), BF16),
                jax.ShapeDtypeStruct((width, ff), BF16),
                jax.ShapeDtypeStruct((width, ff), BF16),
                jax.ShapeDtypeStruct((ff, width), BF16),
            ),
            in_specs=[vmem_spec] * 7,
            out_specs=any_specs,
            scratch_shapes=[pltpu.VMEM((tokens, width), BF16), pltpu.VMEM((tokens, width), BF16), dma((5,))],
            compiler_params=pltpu.CompilerParams(vmem_limit_bytes=4 * 2**20),
        )(*held)
        y_tok, dx_tok, g_up, g_lin, g_down = outs
        return y_tok[None], dx_tok[None], g_up[None, None], g_lin[None, None], g_down[None, None]

    return jax.shard_map(
        device_step,
        mesh=mesh,
        in_specs=(tok_spec, tok_spec, tok_spec, w_spec, w_spec, w_spec, tok_spec),
        out_specs=(tok_spec, tok_spec, w_spec, w_spec, w_spec),
        check_vma=False,
    )
```
